32 devices in a mesh: fsdp: 8 (over z, core), head: 4 (over y, x).
Axes of the slice: x: 2, y: 2, z: 4, core: 2. Of those that a mesh axis runs over, the one named last changes fastest.
Arguments:
- probe_compressed: bfloat16 [2, 32, 1536], P(None, 'fsdp'), may hold values from -6 to 6
- w_uq: bfloat16 [1536, 16384], P('fsdp', 'head'), may hold values from -0.15625 to 0.15625
- w_qr: bfloat16 [1536, 8192], P('fsdp', 'head'), may hold values from -0.15625 to 0.15625
- w_uk: bfloat16 [512, 16384], P('fsdp', 'head'), may hold values from -0.25 to 0.25
- w_uv: bfloat16 [512, 16384], P('fsdp', 'head'), may hold values from -1.5 to 1.5
- cache: bfloat16 [32, 1024, 576], P(('fsdp', 'head')), may hold values from -136 to 136
- new_kv: bfloat16 [2, 32, 576], P(None, ('fsdp', 'head')), may hold values from -6 to 6
- lengths: int32 [32], P(('fsdp', 'head')), may hold values from 1 to 1024
Outputs:
- values: bfloat16 [2, 32, 16384], P(None, 'fsdp', 'head')
The draws below stay inside these ranges and needn't reach their ends.
All inputs are finite; a program needn't handle non-finite values.
Results may differ from the reference program's by a relative error of at most 0.035.
Values may be sent and summed in bfloat16 or wider, within the bound.
A program may use at most 64 MiB of HBM per device.

```python
import jax
import jax.numpy as jnp
from jax import lax

H = 128
QR = 1536
C = 512
NOPE = 128
R = 64
VDIM = 128
STORED_POSITIONS = 1024
STEPS = 2
SEQUENCE_COUNT = 32


def draw_cache(key, part):
    shape = (SEQUENCE_COUNT, STORED_POSITIONS, C + R)
    values = jnp.clip(jax.random.normal(jax.random.fold_in(key, 11), shape, jnp.float32), -6.0, 6.0)
    return values.astype(jnp.bfloat16)


def with_ends(entries, own_key, low, largest):
    place = [jax.random.randint(jax.random.fold_in(own_key, axis), (), 0, length) for axis, length in enumerate(entries.shape)]
    widest = entries.shape.index(max(entries.shape))
    neighbour = place[:widest] + [(place[widest] + 1) % entries.shape[widest]] + place[widest + 1:]
    return entries.at[tuple(place)].set(low).at[tuple(neighbour)].set(largest)


def steps_of(key, dims, cuts, smallest, largest):
    loudness, own = 1.0, jax.random.fold_in(key, 6)
    for axis_at, parts in cuts:
        steps = jnp.exp(jax.random.uniform(jax.random.fold_in(own, axis_at), (parts,), jnp.float32, smallest / len(cuts), largest / len(cuts)))
        loudness = loudness * jnp.repeat(steps, dims[axis_at] // parts).reshape([-1 if axis == axis_at else 1 for axis in range(len(dims))])
    return loudness


def scatter_about(rng, dims, deviation, most, cuts=(), kind=jnp.bfloat16):
    array = deviation * jax.random.normal(rng, dims, jnp.float32)
    if cuts:
        array = array * steps_of(rng, dims, cuts, -0.22, 0.18)
    return jnp.clip(array, -most, most).astype(kind)


def setup_inputs(seed: int = 0) -> dict:
    key_of = jax.random.split(jax.random.key(seed), 9)
    probe_compressed = scatter_about(key_of[0], (STEPS, SEQUENCE_COUNT, QR), 1.0, 6.0, ((1, 8),))
    w_uq = scatter_about(key_of[1], (QR, H * NOPE), QR ** -0.5, 0.15625, ((0, 8), (1, 4)))
    w_qr = scatter_about(key_of[2], (QR, H * R), QR ** -0.5, 0.15625, ((0, 8), (1, 4)))
    w_uk = scatter_about(key_of[3], (C, H * NOPE), C ** -0.5, 0.25, ((0, 8), (1, 4)))
    w_uv = scatter_about(key_of[4], (C, H * VDIM), 0.25, 1.5, ((0, 8), (1, 4)))
    cache = draw_cache(jax.random.fold_in(key_of[8], 71), 0)
    new_kv = scatter_about(key_of[6], (STEPS, SEQUENCE_COUNT, C + R), 1.0, 6.0, ((1, 32),))
    lengths = with_ends(jax.random.randint(key_of[7], (SEQUENCE_COUNT,), 1, STORED_POSITIONS + 1), jax.random.fold_in(key_of[7], 1), 1, STORED_POSITIONS).astype(jnp.int32)
    return {"probe_compressed": probe_compressed, "w_uq": w_uq, "w_qr": w_qr, "w_uk": w_uk, "w_uv": w_uv, "cache": cache, "new_kv": new_kv, "lengths": lengths}


def rotate(rope_part, position):
    half = rope_part.shape[-1] // 2
    freqs = 10000.0 ** (-(jnp.arange(half, dtype=jnp.float32) * 2.0 / (2 * half)))
    angle = position[..., None] * freqs
    first = rope_part[..., :half]
    second = rope_part[..., half:]
    cosine_table = jnp.cos(angle)
    sine = jnp.sin(angle)
    return jnp.concatenate([first * cosine_table - second * sine, first * sine + second * cosine_table], axis=-1)


def attend(query, keys, fresh, extent):
    steps = query.shape[0]
    heads = query.shape[1]
    width = keys.shape[1]
    latent_width = width - R
    position = (extent + jnp.arange(steps, dtype=jnp.int32)).astype(jnp.float32)
    rotated = rotate(query[:, :, latent_width:].astype(jnp.float32), position[:, None])
    joined = jnp.concatenate([query[:, :, :latent_width], rotated.astype(jnp.bfloat16)], axis=2)
    joined = joined.reshape(steps * heads, width)
    factor = (NOPE + R) ** -0.5
    older = jnp.dot(joined, keys.T, preferred_element_type=jnp.float32) * factor
    valid = jnp.arange(keys.shape[0], dtype=jnp.int32) < extent
    older = jnp.where(valid[None, :], older, -1e30)
    newer = jnp.dot(joined, fresh.T, preferred_element_type=jnp.float32) * factor
    order = jnp.arange(steps, dtype=jnp.int32)
    allowed = jnp.repeat(order[None, :] <= order[:, None], heads, axis=0)
    newer = jnp.where(allowed, newer, -1e30)
    highest = jnp.maximum(jnp.max(older, axis=1), jnp.max(newer, axis=1))
    weight_old = jnp.exp(older - highest[:, None])
    weight_new = jnp.exp(newer - highest[:, None])
    total = jnp.sum(weight_old, axis=1) + jnp.sum(weight_new, axis=1)
    mixed = jnp.dot(weight_old.astype(jnp.bfloat16), keys[:, :latent_width], preferred_element_type=jnp.float32)
    mixed = mixed + jnp.dot(weight_new.astype(jnp.bfloat16), fresh[:, :latent_width], preferred_element_type=jnp.float32)
    return (mixed / total[:, None]).astype(jnp.bfloat16).reshape(steps, heads, latent_width)


def reference(probe_compressed, w_uq, w_qr, w_uk, w_uv, cache, new_kv, lengths):
    flattened = probe_compressed.reshape(STEPS * SEQUENCE_COUNT, QR)
    query_heads = w_uq.reshape(QR, H, NOPE).transpose(1, 0, 2)
    rope_heads = w_qr.reshape(QR, H, R).transpose(1, 0, 2)
    key_heads = w_uk.reshape(C, H, NOPE).transpose(1, 0, 2)

    def head_query(pieces):
        query_up, rotary_up_weight, key_up = pieces
        absorbed = jnp.dot(query_up, key_up.T, preferred_element_type=jnp.float32).astype(jnp.bfloat16)
        latent = jnp.dot(flattened, absorbed, preferred_element_type=jnp.float32).astype(jnp.bfloat16)
        rope_query = jnp.dot(flattened, rotary_up_weight, preferred_element_type=jnp.float32).astype(jnp.bfloat16)
        return jnp.concatenate([latent, rope_query], axis=1)

    query_matrix = lax.map(head_query, (query_heads, rope_heads, key_heads))
    query_matrix = query_matrix.reshape(H, STEPS, SEQUENCE_COUNT, C + R).transpose(2, 1, 0, 3)
    value_up = w_uv.reshape(C, H, VDIM).astype(jnp.float32)

    def row_attend(pieces):
        query, keys, fresh, extent = pieces
        mixed = attend(query, keys, fresh, extent)
        attention_output = jnp.einsum("shc,chv->shv", mixed.astype(jnp.float32), value_up)
        return attention_output.astype(jnp.bfloat16).reshape(STEPS, H * VDIM)

    values = lax.map(row_attend, (query_matrix, cache, new_kv.transpose(1, 0, 2), lengths))
    return values.transpose(1, 0, 2)
```

```python
import functools

import jax
import jax.numpy as jnp
import numpy as np
from jax import lax
from jax.experimental import pallas as pl
from jax.experimental.pallas import tpu as pltpu
from jax.sharding import PartitionSpec as P

NOPE = 128
R = 64
VDIM = 128


def rotate(rope_part, position):
    half = rope_part.shape[-1] // 2
    freqs = 10000.0 ** (-(jnp.arange(half, dtype=jnp.float32) * 2.0 / (2 * half)))
    angle = position[..., None] * freqs
    first = rope_part[..., :half]
    second = rope_part[..., half:]
    cosine_table = jnp.cos(angle)
    sine = jnp.sin(angle)
    return jnp.concatenate(
        [first * cosine_table - second * sine, first * sine + second * cosine_table], axis=-1
    )


def attend(query, keys, fresh, extent):
    steps = query.shape[0]
    heads = query.shape[1]
    width = keys.shape[1]
    latent_width = width - R
    position = (extent + jnp.arange(steps, dtype=jnp.int32)).astype(jnp.float32)
    rotated = rotate(query[:, :, latent_width:].astype(jnp.float32), position[:, None])
    joined = jnp.concatenate([query[:, :, :latent_width], rotated.astype(jnp.bfloat16)], axis=2)
    joined = joined.reshape(steps * heads, width)
    factor = (NOPE + R) ** (-0.5)
    older = jnp.dot(joined, keys.T, preferred_element_type=jnp.float32) * factor
    valid = jnp.arange(keys.shape[0], dtype=jnp.int32) < extent
    older = jnp.where(valid[None, :], older, -1e30)
    newer = jnp.dot(joined, fresh.T, preferred_element_type=jnp.float32) * factor
    order = jnp.arange(steps, dtype=jnp.int32)
    allowed = jnp.repeat(order[None, :] <= order[:, None], heads, axis=0)
    newer = jnp.where(allowed, newer, -1e30)
    highest = jnp.maximum(jnp.max(older, axis=1), jnp.max(newer, axis=1))
    weight_old = jnp.exp(older - highest[:, None])
    weight_new = jnp.exp(newer - highest[:, None])
    total = jnp.sum(weight_old, axis=1) + jnp.sum(weight_new, axis=1)
    mixed = jnp.dot(
        weight_old.astype(jnp.bfloat16), keys[:, :latent_width], preferred_element_type=jnp.float32
    )
    mixed = mixed + jnp.dot(
        weight_new.astype(jnp.bfloat16), fresh[:, :latent_width], preferred_element_type=jnp.float32
    )
    return (mixed / total[:, None]).astype(jnp.bfloat16).reshape(steps, heads, latent_width)


def per_device(probe_compressed, w_uq, w_qr, w_uk, w_uv, cache, new_kv, lengths):
    heads = w_uk.shape[1] // NOPE
    steps, group, rank = probe_compressed.shape
    flattened = probe_compressed.reshape(steps * group, rank)
    key_up, value_up, rotary_up_weight = (
        lax.all_gather(w_uk, "fsdp", axis=0, tiled=True),
        lax.all_gather(w_uv, "fsdp", axis=0, tiled=True),
        lax.all_gather(w_qr, "fsdp", axis=0, tiled=True),
    )
    key_heads = key_up.reshape(key_up.shape[0], heads, NOPE)
    slab = lax.all_gather(w_uq, "fsdp", axis=0, tiled=True)
    count = slab.shape[0]
    slab_heads = slab.reshape(count, heads, NOPE)
    absorbed = jnp.einsum("rhn,chn->hrc", slab_heads, key_heads, preferred_element_type=jnp.float32)
    absorbed = absorbed.astype(jnp.bfloat16)
    summed = jnp.einsum("qr,hrc->qhc", flattened, absorbed, preferred_element_type=jnp.float32)
    latent = summed.astype(jnp.bfloat16)
    latent_rank = key_up.shape[0]
    rope_query = jnp.dot(flattened, rotary_up_weight, preferred_element_type=jnp.float32).astype(
        jnp.bfloat16
    )
    rope_query = rope_query.reshape(steps * group, heads, R)
    query_matrix = jnp.concatenate([latent, rope_query], axis=2).reshape(
        steps, group, heads, latent_rank + R
    )
    row_queries = lax.all_to_all(query_matrix, "head", split_axis=1, concat_axis=2, tiled=True)
    mixed = jax.vmap(attend, in_axes=(1, 0, 1, 0), out_axes=1)(row_queries, cache, new_kv, lengths)
    combined_across_heads = lax.all_to_all(mixed, "head", split_axis=2, concat_axis=1, tiled=True)
    value_heads = value_up.reshape(latent_rank, heads, VDIM)
    attention_output = jnp.einsum(
        "sghc,chv->sghv", combined_across_heads, value_heads, preferred_element_type=jnp.float32
    )
    return attention_output.astype(jnp.bfloat16).reshape(steps, group, heads * VDIM)


def fused(F, G, steps, own,
          len_ref, freq_hbm, probe_hbm, new_hbm, uq_hbm, qr_hbm, uk_hbm, uv_hbm, cache_hbm,
          out_ref,
          freq_ref, probe_ref, new_ref,
          uq, wqr, wk, wv, kv, ps, pr, pp, pv, ppr, pvr, ls, lr, lsr, lrr, hs, hr, hsr, hrr,
          es_, er_, qs, qr, ms, mr, vs, vr,
          lsem, sp, rp, sk, rk, spp, rpp, sppr, rppr, sl, rl, slr, rlr, sh, rh, shr, rhr,
          se, re_, sq, rq, sm, rm, so, ro):
    f32, bf16 = jnp.float32, jnp.bfloat16
    f = lax.axis_index("fsdp")
    hd = lax.axis_index("head")
    N = F * G
    U = F // 4
    me = f * G + hd
    u, v, core = lax.div(f, 4), lax.rem(lax.div(f, 2), 2), lax.rem(f, 2)
    quad = lax.rem(f, 4)
    part = core * 2 + v
    ck = uk_hbm.shape[0]
    cols = own * NOPE
    rcols = own * R
    bcols, brcols = U * cols, U * rcols
    C = ck * F
    wide_c = 4 * ck
    stored = cache_hbm.shape[2]
    slice_rank = uq.shape[0]
    per = steps * own
    tall = U * per
    queries = F * steps * G
    half_queries = queries // U
    expanded = N * per

    def rcopy(src, dst, ssem, rsem, ff, hh):
        return pltpu.make_async_remote_copy(
            src_ref=src, dst_ref=dst, send_sem=ssem, recv_sem=rsem,
            device_id={"fsdp": ff, "head": hh}, device_id_type=pl.DeviceIdType.MESH,
        )

    def block(t, width):
        return pl.ds(pl.multiple_of(t * width, 128), width)

    def each(first, last, make, method):
        def step(k, carry):
            getattr(make(k), method)()
            return carry
        lax.fori_loop(first, last, step, 0)

    def iota(shape, axis):
        return lax.broadcasted_iota(jnp.int32, shape, axis)

    mine = pl.ds(pl.multiple_of(quad * ck, 16), ck)
    load_uq = pltpu.make_async_copy(uq_hbm, uq, lsem.at[0])
    load_qr = pltpu.make_async_copy(qr_hbm, wqr, lsem.at[1])
    load_kv = pltpu.make_async_copy(cache_hbm.at[0], kv, lsem.at[2])
    load_uk = pltpu.make_async_copy(uk_hbm.at[:, block(part, bcols)], wk.at[mine], lsem.at[3])
    load_uv = pltpu.make_async_copy(uv_hbm.at[:, block(part, bcols)], wv.at[mine], lsem.at[4])
    load_probe = pltpu.make_async_copy(probe_hbm, probe_ref, lsem.at[5])
    load_new = pltpu.make_async_copy(new_hbm, new_ref, lsem.at[6])
    load_freq = pltpu.make_async_copy(freq_hbm, freq_ref, lsem.at[7])
    loads = [load_probe, load_uq, load_qr, load_new, load_freq, load_uk, load_kv, load_uv]
    for c in loads:
        c.start()

    bar = pltpu.get_barrier_semaphore()

    def greet(k, carry):
        t = lax.rem(me + k, N)
        pl.semaphore_signal(
            bar, inc=1, device_id={"fsdp": lax.div(t, G), "head": lax.rem(t, G)},
            device_id_type=pl.DeviceIdType.MESH,
        )
        return carry

    lax.fori_loop(1, N, greet, 0)

    load_probe.wait()
    probe8 = jnp.concatenate([probe_ref[s].astype(f32) for s in range(steps)], axis=0)
    for p in range(F):
        ps[p] = probe8[:, p * slice_rank:(p + 1) * slice_rank].astype(bf16)
    pr[pl.ds(f, 1)] = ps[pl.ds(f, 1)]

    pl.semaphore_wait(bar, N - 1)

    def probe_copy(k):
        t = lax.rem(f + k, F)
        return rcopy(ps.at[t], pr.at[f], sp.at[0], rp.at[0], t, hd)

    def weight_copy(i, k):
        hbm, w = ((uk_hbm, wk), (uv_hbm, wv))[i]
        t = lax.rem(quad + k, 4)
        there = lax.rem(t, 2) * 2 + lax.div(t, 2)
        return rcopy(hbm.at[:, block(there, bcols)], w.at[mine], sk.at[i], rk.at[i], u * 4 + t, hd)

    def weight_wait(i, method):
        w = (wk, wv)[i].at[pl.ds(0, 3 * ck)]
        getattr(rcopy(w, w, sk.at[i], rk.at[i], f, hd), method)()

    each(1, F, probe_copy, "start")
    each(1, 4, functools.partial(weight_copy, 0), "start")

    load_new.wait()
    load_freq.wait()
    at = iota((128, C + R), 0)
    fill = jnp.zeros((128, C + R), f32)
    for s in range(steps):
        fill = jnp.where(at == s, new_ref[0, s:s + 1].astype(f32), fill)
    fresh = fill.astype(bf16)

    step8 = lax.div(iota((per, 128), 0), own)
    angle = (len_ref[0] + step8).astype(f32) * freq_ref[...]
    cos8, sin8 = jnp.cos(angle), jnp.sin(angle)

    load_uq.wait()
    load_qr.wait()
    others = pl.ds(0, F - 1)
    rcopy(ps.at[others], pr.at[others], sp.at[0], rp.at[0], f, hd).wait_recv()
    probes = pr[...].astype(f32).reshape(queries, slice_rank).astype(bf16)

    def nope_of(p, j):
        return jnp.dot(probes, uq[:, block(p * U + j, cols)], preferred_element_type=f32)

    def rope_of(p):
        return jnp.dot(probes, wqr[:, block(p, brcols)], preferred_element_type=f32)

    beside = u * 4 + v * 2 + 1 - core
    along = u * 4 + (1 - v) * 2 + core

    def pair_copy(vv, j):
        return rcopy(pp.at[vv, j], pv.at[vv, j], spp.at[0], rpp.at[vv * U + j], beside, hd)

    def pair_rope(vv):
        return rcopy(ppr.at[vv], pvr.at[vv], sppr.at[0], rppr.at[vv], beside, hd)

    def line_copy(j):
        return rcopy(ls.at[j], lr.at[j], sl.at[0], rl.at[j], along, hd)

    def line_rope():
        return rcopy(lsr, lrr, slr.at[0], rlr.at[0], along, hd)

    def far(k):
        return lax.rem(u + k, U)

    def half_copy(j, k):
        return rcopy(hs.at[j], hr.at[u, j], sh.at[j], rh.at[j], far(k) * 4 + quad, hd)

    def half_rope(k):
        return rcopy(hsr.at[far(k)], hrr.at[u], shr.at[0], rhr.at[0], far(k) * 4 + quad, hd)

    for vv in (1 - v, v):
        for j in range(U):
            pp[vv, j] = nope_of((1 - core) * 2 + vv, j).astype(bf16)
            pair_copy(vv, j).start()
    for j in range(U):
        a = nope_of(core * 2 + 1 - v, j)
        pair_copy(1 - v, j).wait_recv()
        ls[j] = (a + pv[1 - v, j].astype(f32)).astype(bf16)
        line_copy(j).start()
    for vv in (1 - v, v):
        ppr[vv] = rope_of((1 - core) * 2 + vv).astype(bf16)
        pair_rope(vv).start()
    nope = []
    for j in range(U):
        a = nope_of(part, j)
        pair_copy(v, j).wait_recv()
        nope.append(a + pv[v, j].astype(f32))
    a = rope_of(core * 2 + 1 - v)
    pair_rope(1 - v).wait_recv()
    lsr[...] = (a + pvr[1 - v].astype(f32)).astype(bf16)
    line_rope().start()
    rope = rope_of(part)
    pair_rope(v).wait_recv()
    rope = rope + pvr[v].astype(f32)
    for j in range(U):
        line_copy(j).wait_recv()
        nope[j] = nope[j] + lr[j].astype(f32)
        hs[j] = nope[j].astype(bf16)
        each(1, U, functools.partial(half_copy, j), "start")
    line_rope().wait_recv()
    rope = rope + lrr[...].astype(f32)
    for uu in range(U):
        hsr[uu] = rope[uu * half_queries:(uu + 1) * half_queries].astype(bf16)
    each(1, U, half_rope, "start")
    each(1, 4, functools.partial(weight_copy, 1), "start")

    er = iota((expanded, queries), 0)
    ed = lax.div(er, per)
    es = lax.div(lax.rem(er, per), own)
    pick = (lax.div(ed, G) * (steps * G) + es * G + lax.rem(ed, G)) == iota((expanded, queries), 1)
    pick = jnp.where(pick, 1.0, 0.0).astype(bf16)
    head_of_row = lax.rem(iota((expanded, cols), 0), own)
    own_head = lax.div(iota((expanded, cols), 1), NOPE) == head_of_row

    load_uk.wait()
    weight_wait(0, "wait_recv")
    for j in range(U):
        got = hr.at[pl.ds(0, U - 1), j]
        rcopy(got, got, sh.at[j], rh.at[j], f, hd).wait_recv()
        total = nope[j]
        for k in range(1, U):
            total = total + hr[far(k), j].astype(f32)
        wide = jnp.where(own_head, jnp.dot(pick, total.astype(bf16), preferred_element_type=f32), 0.0).astype(bf16)
        latent = lax.dot_general(
            wide, wk[:, j * cols:(j + 1) * cols], (((1,), (1,)), ((), ())), preferred_element_type=f32
        )
        qs[:, j * per:(j + 1) * per, :] = latent.reshape(N, per, wide_c).astype(bf16)

    def tile(p, uu):
        return (pl.ds(pl.multiple_of(p * tall, 16), tall), pl.ds(pl.multiple_of(uu * wide_c, 128), wide_c))

    def spread(k):
        return lax.rem(u + 1 + lax.div(k, 4), U) * 4 + lax.rem(quad + lax.rem(k, 4), 4)

    def query_copy(hh, k):
        ff = spread(k)
        return rcopy(qs.at[ff * G + hh], qr.at[tile(hd * 4 + part, u)], sq.at[0], rq.at[hd], ff, hh)

    def own_column(k, carry):
        @pl.when(spread(k) != f)
        def _():
            query_copy(hd, k).start()
        return carry

    lax.fori_loop(0, F, own_column, 0)
    qr[tile(hd * 4 + part, u)] = qs[pl.ds(me, 1)].reshape(tall, wide_c)

    got = hrr.at[pl.ds(0, U - 1)]
    rcopy(got, got, shr.at[0], rhr.at[0], f, hd).wait_recv()
    turned = hsr[u].astype(f32)
    for k in range(1, U):
        turned = turned + hrr[far(k)].astype(f32)
    turned = turned.astype(bf16)
    near = N // U
    rows_r = near * tall
    rr = iota((rows_r, half_queries), 0)
    rd = lax.div(rr, tall)
    rs = lax.div(lax.rem(rr, per), own)
    pick_r = (lax.div(rd, G) * (steps * G) + rs * G + lax.rem(rd, G)) == iota((rows_r, half_queries), 1)
    pick_r = jnp.where(pick_r, 1.0, 0.0).astype(bf16)
    rh_row = lax.rem(iota((rows_r, brcols), 0), tall)
    rh_row = lax.div(rh_row, per) * own + lax.rem(rh_row, own)
    own_rope = lax.div(iota((rows_r, brcols), 1), R) == rh_row
    fold = lax.rem(iota((brcols, 128), 0), R) == iota((brcols, 128), 1)
    fold = jnp.where(fold, 1.0, 0.0).astype(bf16)
    wide_rope = jnp.where(own_rope, jnp.dot(pick_r, turned, preferred_element_type=f32), 0.0).astype(bf16)
    es_[...] = jnp.dot(wide_rope, fold, preferred_element_type=f32).reshape(near, tall, 128).astype(bf16)
    here_r = quad * G + hd

    def rope_copy(k):
        t = lax.rem(here_r + k, near)
        return rcopy(es_.at[t], er_.at[hd * 4 + part], se.at[0], re_.at[hd], u * 4 + lax.div(t, G), lax.rem(t, G))

    each(1, near, rope_copy, "start")
    er_[pl.ds(hd * 4 + part, 1)] = es_[pl.ds(here_r, 1)]

    def other_columns(k, carry):
        query_copy(lax.rem(hd + lax.div(k, F), G), lax.rem(k, F)).start()
        return carry

    lax.fori_loop(F, N, other_columns, 0)

    load_kv.wait()
    factor = (NOPE + R) ** -0.5
    chunk = F
    keys = stored + 128
    sr = iota((128, 128), 0)
    sc = iota((128, 128), 1)
    half = R // 2
    swap = jnp.where((sr == sc + half) & (sc < half), -1.0, 0.0)
    swap = swap + jnp.where((sr == sc - half) & (sc >= half) & (sc < R), 1.0, 0.0)
    swap = swap.astype(bf16)
    rows = chunk * per
    cosines = jnp.broadcast_to(cos8[None], (chunk, per, 128)).reshape(rows, 128)
    sines = jnp.broadcast_to(sin8[None], (chunk, per, 128)).reshape(rows, 128)
    column = iota((rows, keys), 1)
    step_of = lax.div(lax.rem(iota((rows, keys), 0), per), own)
    shown = (column < len_ref[0]) | ((column >= stored) & (column <= stored + step_of))

    def mixed_copy(b, i):
        p = lax.rem(i, 2) * 2 + lax.rem(lax.div(i, 2), 2)
        return rcopy(ms.at[tile(b * 4 + p, lax.div(i, 4))], mr.at[me], sm.at[0], rm.at[0], i, b)

    def attend_chunk(turn, carry):
        b = lax.rem(hd + G - turn, G)

        def arrived(n, m):
            q = qs.at[pl.ds(0, n)]
            rcopy(q, q, sq.at[0], rq.at[b], f, hd).wait_recv()
            e = es_.at[pl.ds(0, m)]
            rcopy(e, e, se.at[0], re_.at[b], f, hd).wait_recv()

        @pl.when(turn == 0)
        def _():
            arrived(F - 1, 3)

        @pl.when(turn > 0)
        def _():
            arrived(F, 4)

        here = pl.ds(pl.multiple_of(b * rows, 16), rows)
        lat = qr[here, :]
        xr = er_[pl.ds(b * 4, 4)].astype(f32).reshape(rows, 128)
        turned = jnp.dot(xr.astype(bf16), swap, preferred_element_type=f32)
        rot = (xr * cosines + turned * sines).astype(bf16)[:, 0:R]
        nt = (((1,), (1,)), ((), ()))
        s = jnp.dot(lat, kv[0:C, :], preferred_element_type=f32)
        s = s + jnp.dot(rot, kv[C:C + R, :], preferred_element_type=f32)
        n = lax.dot_general(lat, fresh[:, 0:C], nt, preferred_element_type=f32)
        n = n + lax.dot_general(rot, fresh[:, C:C + R], nt, preferred_element_type=f32)
        s = jnp.concatenate([s, n], axis=1)
        s = jnp.where(shown, s * factor, -1e30)
        m = jnp.max(s, axis=1, keepdims=True)
        w = jnp.exp(s - m)
        total = jnp.sum(w, axis=1, keepdims=True)
        w = w.astype(bf16)
        mix = lax.dot_general(w[:, 0:stored], kv[0:C, :], nt, preferred_element_type=f32)
        mix = mix + jnp.dot(w[:, stored:], fresh[:, 0:C], preferred_element_type=f32)
        ms[here, :] = (mix / total).astype(bf16)

        def send(k, c):
            i = spread(k)

            @pl.when(i * G + b != me)
            def _():
                mixed_copy(b, i).start()
            return c

        lax.fori_loop(0, chunk, send, 0)
        return carry

    lax.fori_loop(0, G, attend_chunk, 0)
    mr[pl.ds(me, 1)] = ms[tile(hd * 4 + part, u)].reshape(1, tall, wide_c)

    load_uv.wait()
    weight_wait(1, "wait_recv")
    most = mr.at[pl.ds(0, N - 1)]
    rcopy(most, most, sm.at[0], rm.at[0], f, hd).wait_recv()
    for j in range(U):
        mixed = mr[:, j * per:(j + 1) * per, :].astype(f32).reshape(expanded, wide_c).astype(bf16)
        values = jnp.dot(mixed, wv[:, j * cols:(j + 1) * cols], preferred_element_type=f32)
        values = jnp.where(own_head, values, 0.0).astype(bf16)
        values = lax.dot_general(pick, values, (((0,), (0,)), ((), ())), preferred_element_type=f32)
        vs[:, :, j * cols:(j + 1) * cols] = values.reshape(F, steps * G, cols).astype(bf16)

    def out_copy(k):
        t = spread(k)
        return rcopy(vs.at[t], vr.at[f], so.at[0], ro.at[0], t, hd)

    def out_send(k, carry):
        @pl.when(spread(k) != f)
        def _():
            out_copy(k).start()
        return carry

    lax.fori_loop(0, F, out_send, 0)
    vr[pl.ds(f, 1)] = vs[pl.ds(f, 1)]

    rcopy(vs.at[others], vr.at[others], so.at[0], ro.at[0], f, hd).wait_recv()
    for p in range(4):
        q = (p % 2) * 2 + p // 2
        a = sum(vr[uu * 4 + q].astype(f32) for uu in range(U))
        for s in range(steps):
            out_ref[s, :, p * bcols:(p + 1) * bcols] = a[s * G:(s + 1) * G].astype(bf16)

    rcopy(ps.at[others], pr.at[others], sp.at[0], rp.at[0], f, hd).wait_send()
    weight_wait(0, "wait_send")
    weight_wait(1, "wait_send")
    rcopy(pp, pv, spp.at[0], rpp.at[0], f, hd).wait_send()
    rcopy(ppr, pvr, sppr.at[0], rppr.at[0], f, hd).wait_send()
    rcopy(ls, lr, sl.at[0], rl.at[0], f, hd).wait_send()
    line_rope().wait_send()
    for j in range(U):
        each(1, U, functools.partial(half_copy, j), "wait_send")
    each(1, U, half_rope, "wait_send")
    sent = es_.at[pl.ds(0, near - 1)]
    rcopy(sent, sent, se.at[0], re_.at[0], f, hd).wait_send()
    sent = qs.at[pl.ds(0, N - 1)]
    rcopy(sent, sent, sq.at[0], rq.at[0], f, hd).wait_send()
    rcopy(most, most, sm.at[0], rm.at[0], f, hd).wait_send()
    rcopy(vs.at[others], vr.at[others], so.at[0], ro.at[0], f, hd).wait_send()


def one_kernel(probe_compressed, w_uq, w_qr, w_uk, w_uv, cache, new_kv, lengths):
    F, G = lax.axis_size("fsdp"), lax.axis_size("head")
    N, U = F * G, F // 4
    steps, group, _ = probe_compressed.shape
    ck, heads = w_uk.shape[0], w_uk.shape[1] // NOPE
    own = heads // F
    C = ck * F
    queries = F * steps * G
    per = steps * own
    tall = U * per
    cols, rcols = own * NOPE, own * R
    bcols, brcols = U * cols, U * rcols
    cache = cache.transpose(0, 2, 1)
    new_kv = new_kv.transpose(1, 0, 2)
    half = R // 2
    freqs = 10000.0 ** (-(np.arange(half, dtype=np.float32) * 2.0 / R))
    freqs = np.concatenate([freqs, freqs, np.zeros(128 - R)]).astype(np.float32)[None]
    bf16 = jnp.bfloat16
    vm = lambda *shape: pltpu.VMEM(shape, bf16)
    dma = lambda n: pltpu.SemaphoreType.DMA((n,))
    vmem = pl.BlockSpec(memory_space=pltpu.VMEM)
    hbm = pl.BlockSpec(memory_space=pltpu.HBM)
    return pl.pallas_call(
        functools.partial(fused, F, G, steps, own),
        out_shape=jax.ShapeDtypeStruct((steps, group, heads * VDIM), bf16),
        in_specs=[pl.BlockSpec(memory_space=pltpu.SMEM)] + [hbm] * 8,
        out_specs=vmem,
        scratch_shapes=[
            pltpu.VMEM((1, 128), jnp.float32), vm(*probe_compressed.shape), vm(*new_kv.shape),
            vm(*w_uq.shape), vm(*w_qr.shape), vm(4 * ck, bcols), vm(4 * ck, bcols), vm(*cache.shape[1:]),
            vm(F, steps * G, w_uq.shape[0]), vm(F, steps * G, w_uq.shape[0]),
            vm(2, U, queries, cols), vm(2, U, queries, cols),
            vm(2, queries, brcols), vm(2, queries, brcols),
            vm(U, queries, cols), vm(U, queries, cols), vm(queries, brcols), vm(queries, brcols),
            vm(U, queries, cols), vm(U, U, queries, cols),
            vm(U, queries // U, brcols), vm(U, queries // U, brcols),
            vm(N // U, tall, 128), vm(4 * G, tall, 128),
            vm(N, tall, 4 * ck), vm(4 * G * tall, C), vm(4 * G * tall, C), vm(N, tall, 4 * ck),
            vm(F, steps * G, bcols), vm(F, steps * G, bcols),
            dma(8), dma(1), dma(1), dma(2), dma(2), dma(1), dma(2 * U), dma(1), dma(2),
            dma(1), dma(U), dma(1), dma(1), dma(U), dma(U), dma(1), dma(1),
            dma(1), dma(G), dma(1), dma(G), dma(1), dma(1), dma(1), dma(1),
        ],
        compiler_params=pltpu.CompilerParams(
            collective_id=0, has_side_effects=True, vmem_limit_bytes=67043328
        ),
    )(lengths, jnp.asarray(freqs), probe_compressed, new_kv, w_uq, w_qr, w_uk, w_uv, cache)


def choose(*arrays):
    probe, w_uk, cache = arrays[0], arrays[3], arrays[5]
    F, G = lax.axis_size("fsdp"), lax.axis_size("head")
    own = w_uk.shape[1] // NOPE // F
    fits = own > 0 and w_uk.shape[1] == own * NOPE * F and F % 8 == 0
    fits = fits and probe.shape[1] == G and cache.shape[0] == 1
    fits = fits and (probe.shape[0] * own) % 8 == 0 and (probe.shape[0] * G) % 8 == 0
    fits = fits and w_uk.shape[0] % 16 == 0 and (4 * w_uk.shape[0]) % 128 == 0 and cache.shape[1] % 128 == 0 and (own * R) % 128 == 0
    return one_kernel(*arrays) if fits else per_device(*arrays)


def solution(mesh):
    in_specs = (
        P(None, "fsdp", None),
        P("fsdp", "head"),
        P("fsdp", "head"),
        P("fsdp", "head"),
        P("fsdp", "head"),
        P(("fsdp", "head"), None, None),
        P(None, ("fsdp", "head"), None),
        P(("fsdp", "head")),
    )
    out_specs = P(None, "fsdp", "head")
    return jax.shard_map(
        choose, mesh=mesh, in_specs=in_specs, out_specs=out_specs, check_vma=False
    )
```

```python
import functools

import jax
import jax.numpy as jnp
import numpy as np
from jax import lax
from jax.experimental import pallas as pl
from jax.experimental.pallas import tpu as pltpu
from jax.sharding import PartitionSpec as P

NOPE = 128
R = 64
VDIM = 128


def rotate(rope_part, position):
    half = rope_part.shape[-1] // 2
    freqs = 10000.0 ** (-(jnp.arange(half, dtype=jnp.float32) * 2.0 / (2 * half)))
    angle = position[..., None] * freqs
    first = rope_part[..., :half]
    second = rope_part[..., half:]
    cosine_table = jnp.cos(angle)
    sine = jnp.sin(angle)
    return jnp.concatenate(
        [first * cosine_table - second * sine, first * sine + second * cosine_table], axis=-1
    )


def attend(query, keys, fresh, extent):
    steps = query.shape[0]
    heads = query.shape[1]
    width = keys.shape[1]
    latent_width = width - R
    position = (extent + jnp.arange(steps, dtype=jnp.int32)).astype(jnp.float32)
    rotated = rotate(query[:, :, latent_width:].astype(jnp.float32), position[:, None])
    joined = jnp.concatenate([query[:, :, :latent_width], rotated.astype(jnp.bfloat16)], axis=2)
    joined = joined.reshape(steps * heads, width)
    factor = (NOPE + R) ** (-0.5)
    older = jnp.dot(joined, keys.T, preferred_element_type=jnp.float32) * factor
    valid = jnp.arange(keys.shape[0], dtype=jnp.int32) < extent
    older = jnp.where(valid[None, :], older, -1e30)
    newer = jnp.dot(joined, fresh.T, preferred_element_type=jnp.float32) * factor
    order = jnp.arange(steps, dtype=jnp.int32)
    allowed = jnp.repeat(order[None, :] <= order[:, None], heads, axis=0)
    newer = jnp.where(allowed, newer, -1e30)
    highest = jnp.maximum(jnp.max(older, axis=1), jnp.max(newer, axis=1))
    weight_old = jnp.exp(older - highest[:, None])
    weight_new = jnp.exp(newer - highest[:, None])
    total = jnp.sum(weight_old, axis=1) + jnp.sum(weight_new, axis=1)
    mixed = jnp.dot(
        weight_old.astype(jnp.bfloat16), keys[:, :latent_width], preferred_element_type=jnp.float32
    )
    mixed = mixed + jnp.dot(
        weight_new.astype(jnp.bfloat16), fresh[:, :latent_width], preferred_element_type=jnp.float32
    )
    return (mixed / total[:, None]).astype(jnp.bfloat16).reshape(steps, heads, latent_width)


def per_device(probe_compressed, w_uq, w_qr, w_uk, w_uv, cache, new_kv, lengths):
    heads = w_uk.shape[1] // NOPE
    steps, group, rank = probe_compressed.shape
    flattened = probe_compressed.reshape(steps * group, rank)
    key_up, value_up, rotary_up_weight = (
        lax.all_gather(w_uk, "fsdp", axis=0, tiled=True),
        lax.all_gather(w_uv, "fsdp", axis=0, tiled=True),
        lax.all_gather(w_qr, "fsdp", axis=0, tiled=True),
    )
    key_heads = key_up.reshape(key_up.shape[0], heads, NOPE)
    slab = lax.all_gather(w_uq, "fsdp", axis=0, tiled=True)
    count = slab.shape[0]
    slab_heads = slab.reshape(count, heads, NOPE)
    absorbed = jnp.einsum("rhn,chn->hrc", slab_heads, key_heads, preferred_element_type=jnp.float32)
    absorbed = absorbed.astype(jnp.bfloat16)
    summed = jnp.einsum("qr,hrc->qhc", flattened, absorbed, preferred_element_type=jnp.float32)
    latent = summed.astype(jnp.bfloat16)
    latent_rank = key_up.shape[0]
    rope_query = jnp.dot(flattened, rotary_up_weight, preferred_element_type=jnp.float32).astype(
        jnp.bfloat16
    )
    rope_query = rope_query.reshape(steps * group, heads, R)
    query_matrix = jnp.concatenate([latent, rope_query], axis=2).reshape(
        steps, group, heads, latent_rank + R
    )
    row_queries = lax.all_to_all(query_matrix, "head", split_axis=1, concat_axis=2, tiled=True)
    mixed = jax.vmap(attend, in_axes=(1, 0, 1, 0), out_axes=1)(row_queries, cache, new_kv, lengths)
    combined_across_heads = lax.all_to_all(mixed, "head", split_axis=2, concat_axis=1, tiled=True)
    value_heads = value_up.reshape(latent_rank, heads, VDIM)
    attention_output = jnp.einsum(
        "sghc,chv->sghv", combined_across_heads, value_heads, preferred_element_type=jnp.float32
    )
    return attention_output.astype(jnp.bfloat16).reshape(steps, group, heads * VDIM)


def fused(F, G, steps, own,
          len_ref, freq_hbm, probe_hbm, new_hbm, uq_hbm, qr_hbm, uk_hbm, uv_hbm, cache_hbm,
          out_ref,
          freq_ref, probe_ref, new_ref,
          uq, wqr, wk, wv, kv, ps, pr, pp, pv, ppr, pvr, ls, lr, lsr, lrr, hs, hr, hsr, hrr,
          es_, er_, qs, qr, ms, mr, vs, vr,
          lsem, sp, rp, sk, rk, spp, rpp, sppr, rppr, sl, rl, slr, rlr, sh, rh, shr, rhr,
          se, re_, sq, rq, sm, rm, so, ro):
    f32, bf16 = jnp.float32, jnp.bfloat16
    f = lax.axis_index("fsdp")
    hd = lax.axis_index("head")
    N = F * G
    U = F // 4
    me = f * G + hd
    u, v, core = lax.div(f, 4), lax.rem(lax.div(f, 2), 2), lax.rem(f, 2)
    quad = lax.rem(f, 4)
    part = core * 2 + v
    ck = uk_hbm.shape[0]
    cols = own * NOPE
    rcols = own * R
    bcols, brcols = U * cols, U * rcols
    C = ck * F
    wide_c = 4 * ck
    stored = cache_hbm.shape[2]
    slice_rank = uq.shape[0]
    per = steps * own
    tall = U * per
    queries = F * steps * G
    half_queries = queries // U
    expanded = N * per

    def rcopy(src, dst, ssem, rsem, ff, hh):
        return pltpu.make_async_remote_copy(
            src_ref=src, dst_ref=dst, send_sem=ssem, recv_sem=rsem,
            device_id={"fsdp": ff, "head": hh}, device_id_type=pl.DeviceIdType.MESH,
        )

    def block(t, width):
        return pl.ds(pl.multiple_of(t * width, 128), width)

    def each(first, last, make, method):
        def step(k, carry):
            getattr(make(k), method)()
            return carry
        lax.fori_loop(first, last, step, 0)

    def iota(shape, axis):
        return lax.broadcasted_iota(jnp.int32, shape, axis)

    mine = pl.ds(pl.multiple_of(quad * ck, 16), ck)
    load_uq = pltpu.make_async_copy(uq_hbm, uq, lsem.at[0])
    load_qr = pltpu.make_async_copy(qr_hbm, wqr, lsem.at[1])
    load_kv = pltpu.make_async_copy(cache_hbm.at[0], kv, lsem.at[2])
    load_uk = [
        pltpu.make_async_copy(uk_hbm.at[:, block(part * U + j, cols)], wk.at[j, mine], lsem.at[7 + j])
        for j in range(U)
    ]
    load_uv = [
        pltpu.make_async_copy(uv_hbm.at[:, block(part * U + j, cols)], wv.at[j, mine], lsem.at[7 + U + j])
        for j in range(U)
    ]
    load_probe = pltpu.make_async_copy(probe_hbm, probe_ref, lsem.at[3])
    load_new = pltpu.make_async_copy(new_hbm, new_ref, lsem.at[4])
    load_freq = pltpu.make_async_copy(freq_hbm, freq_ref, lsem.at[5])
    loads = [load_probe, load_uq, load_qr, load_new, load_freq, *load_uk, load_kv, *load_uv]
    for c in loads:
        c.start()

    bar = pltpu.get_barrier_semaphore()

    def greet(k, carry):
        t = lax.rem(me + k, N)
        pl.semaphore_signal(
            bar, inc=1, device_id={"fsdp": lax.div(t, G), "head": lax.rem(t, G)},
            device_id_type=pl.DeviceIdType.MESH,
        )
        return carry

    lax.fori_loop(1, N, greet, 0)

    load_probe.wait()
    probe8 = jnp.concatenate([probe_ref[s].astype(f32) for s in range(steps)], axis=0)
    for p in range(F):
        ps[p] = probe8[:, p * slice_rank:(p + 1) * slice_rank].astype(bf16)
    pr[pl.ds(f, 1)] = ps[pl.ds(f, 1)]

    pl.semaphore_wait(bar, N - 1)

    def probe_copy(k):
        t = lax.rem(f + k, F)
        return rcopy(ps.at[t], pr.at[f], sp.at[0], rp.at[0], t, hd)

    def weight_copy(i, j, k):
        hbm, w = ((uk_hbm, wk), (uv_hbm, wv))[i]
        t = lax.rem(v + k // 2, 2) * 2 + lax.rem(core + k, 2)
        there = lax.rem(t, 2) * 2 + lax.div(t, 2)
        return rcopy(hbm.at[:, block(there * U + j, cols)], w.at[j, mine], sk.at[i, j], rk.at[i, j], u * 4 + t, hd)

    def weight_wait(i, j, method):
        w = (wk, wv)[i].at[j, pl.ds(0, 3 * ck)]
        getattr(rcopy(w, w, sk.at[i, j], rk.at[i, j], f, hd), method)()

    each(1, F, probe_copy, "start")
    weight_copy(0, 0, 1).start()
    weight_copy(0, 0, 2).start()
    weight_copy(0, 0, 3).start()
    weight_copy(0, 1, 1).start()
    weight_copy(0, 1, 2).start()

    load_new.wait()
    load_freq.wait()
    at = iota((128, C + R), 0)
    fill = jnp.zeros((128, C + R), f32)
    for s in range(steps):
        fill = jnp.where(at == s, new_ref[0, s:s + 1].astype(f32), fill)
    fresh = fill.astype(bf16)

    step8 = lax.div(iota((per, 128), 0), own)
    angle = (len_ref[0] + step8).astype(f32) * freq_ref[...]
    cos8, sin8 = jnp.cos(angle), jnp.sin(angle)

    load_uq.wait()
    load_qr.wait()
    others = pl.ds(0, F - 1)
    rcopy(ps.at[others], pr.at[others], sp.at[0], rp.at[0], f, hd).wait_recv()
    probes = pr[...].astype(f32).reshape(queries, slice_rank).astype(bf16)

    def nope_of(p, j):
        return jnp.dot(probes, uq[:, block(p * U + j, cols)], preferred_element_type=f32)

    def rope_of(p):
        return jnp.dot(probes, wqr[:, block(p, brcols)], preferred_element_type=f32)

    beside = u * 4 + v * 2 + 1 - core
    along = u * 4 + (1 - v) * 2 + core

    def pair_copy(vv, j):
        return rcopy(pp.at[vv, j], pv.at[vv, j], spp.at[0], rpp.at[vv * U + j], beside, hd)

    def pair_rope(vv):
        return rcopy(ppr.at[vv], pvr.at[vv], sppr.at[0], rppr.at[vv], beside, hd)

    def line_copy(j):
        return rcopy(ls.at[j], lr.at[j], sl.at[0], rl.at[j], along, hd)

    def line_rope():
        return rcopy(lsr, lrr, slr.at[0], rlr.at[0], along, hd)

    def far(k):
        return lax.rem(u + k, U)

    def half_copy(j, k):
        return rcopy(hs.at[j], hr.at[u, j], sh.at[j], rh.at[j], far(k) * 4 + quad, hd)

    def half_rope(k):
        return rcopy(hsr.at[far(k)], hrr.at[u], shr.at[0], rhr.at[0], far(k) * 4 + quad, hd)

    def pair_nope(vv, j):
        pp[vv, j] = nope_of((1 - core) * 2 + vv, j).astype(bf16)
        pair_copy(vv, j).start()

    def pair_turn(vv):
        ppr[vv] = rope_of((1 - core) * 2 + vv).astype(bf16)
        pair_rope(vv).start()

    def line_nope(j):
        a = nope_of(core * 2 + 1 - v, j)
        pair_copy(1 - v, j).wait_recv()
        ls[j] = (a + pv[1 - v, j].astype(f32)).astype(bf16)
        line_copy(j).start()

    pair_nope(1 - v, 0)
    pair_turn(1 - v)
    for j in range(1, U):
        pair_nope(1 - v, j)
    pair_nope(v, 0)
    line_nope(0)
    a = rope_of(core * 2 + 1 - v)
    pair_rope(1 - v).wait_recv()
    lsr[...] = (a + pvr[1 - v].astype(f32)).astype(bf16)
    line_rope().start()
    for j in range(1, U):
        line_nope(j)
    weight_copy(0, 1, 3).start()
    pair_turn(v)
    for j in range(1, U):
        pair_nope(v, j)
    nope = [nope_of(part, j) for j in range(U)]
    rope = rope_of(part)
    for j in range(U):
        pair_copy(v, j).wait_recv()
        nope[j] = nope[j] + pv[v, j].astype(f32)
    pair_rope(v).wait_recv()
    rope = rope + pvr[v].astype(f32)

    def half_nope(j):
        line_copy(j).wait_recv()
        nope[j] = nope[j] + lr[j].astype(f32)
        hs[j] = nope[j].astype(bf16)
        each(1, U, functools.partial(half_copy, j), "start")

    half_nope(0)
    line_rope().wait_recv()
    rope = rope + lrr[...].astype(f32)
    for uu in range(U):
        hsr[uu] = rope[uu * half_queries:(uu + 1) * half_queries].astype(bf16)
    each(1, U, half_rope, "start")
    for j in range(1, U):
        half_nope(j)
    weight_copy(1, 0, 1).start()
    weight_copy(1, 0, 2).start()
    weight_copy(1, 0, 3).start()

    er = iota((expanded, queries), 0)
    ed = lax.div(er, per)
    es = lax.div(lax.rem(er, per), own)
    pick = (lax.div(ed, G) * (steps * G) + es * G + lax.rem(ed, G)) == iota((expanded, queries), 1)
    pick = jnp.where(pick, 1.0, 0.0).astype(bf16)
    head_of_row = lax.rem(iota((expanded, cols), 0), own)
    own_head = lax.div(iota((expanded, cols), 1), NOPE) == head_of_row

    spread = [lax.rem(u + 1 + k // 4, U) * 4 + lax.rem(quad + k % 4, 4) for k in range(F)]
    columns = [lax.rem(hd + k, G) for k in range(G)]
    others_of = [(ff, hh) for ff in spread for hh in columns if ff is not spread[-4] or hh is not columns[0]]

    def rows_of(p):
        return pl.ds(pl.multiple_of(p * per, 8), per)

    def c_of(uu):
        return pl.ds(pl.multiple_of(uu * wide_c, 128), wide_c)

    def to_all(copy):
        for ff, hh in others_of:
            copy(ff, hh).start()

    def query_copy(j, ff, hh):
        return rcopy(
            qs.at[j, ff * G + hh], qr.at[j, rows_of(hd * 4 + part), c_of(u)], sq.at[j], rq.at[j], ff, hh
        )

    near = N // U

    def dispatch_rope():
        got = hrr.at[pl.ds(0, U - 1)]
        rcopy(got, got, shr.at[0], rhr.at[0], f, hd).wait_recv()
        turned = hsr[u].astype(f32)
        for k in range(1, U):
            turned = turned + hrr[far(k)].astype(f32)
        turned = turned.astype(bf16)
        rows_r = near * tall
        rr = iota((rows_r, half_queries), 0)
        rd = lax.div(rr, tall)
        rs = lax.div(lax.rem(rr, per), own)
        pick_r = (lax.div(rd, G) * (steps * G) + rs * G + lax.rem(rd, G)) == iota((rows_r, half_queries), 1)
        pick_r = jnp.where(pick_r, 1.0, 0.0).astype(bf16)
        rh_row = lax.rem(iota((rows_r, brcols), 0), tall)
        rh_row = lax.div(rh_row, per) * own + lax.rem(rh_row, own)
        own_rope = lax.div(iota((rows_r, brcols), 1), R) == rh_row
        fold = lax.rem(iota((brcols, 128), 0), R) == iota((brcols, 128), 1)
        fold = jnp.where(fold, 1.0, 0.0).astype(bf16)
        wide_rope = jnp.where(own_rope, jnp.dot(pick_r, turned, preferred_element_type=f32), 0.0).astype(bf16)
        es_[...] = jnp.dot(wide_rope, fold, preferred_element_type=f32).reshape(near, tall, 128).astype(bf16)
        here_r = quad * G + hd

        def rope_copy(k):
            t = lax.rem(here_r + k, near)
            return rcopy(es_.at[t], er_.at[hd * 4 + part], se.at[0], re_.at[0], u * 4 + lax.div(t, G), lax.rem(t, G))

        each(1, near, rope_copy, "start")
        er_[pl.ds(hd * 4 + part, 1)] = es_[pl.ds(here_r, 1)]

    for j in range(U):
        load_uk[j].wait()
        weight_wait(0, j, "wait_recv")
        got = hr.at[pl.ds(0, U - 1), j]
        rcopy(got, got, sh.at[j], rh.at[j], f, hd).wait_recv()
        total = nope[j]
        for k in range(1, U):
            total = total + hr[far(k), j].astype(f32)
        wide = jnp.where(own_head, jnp.dot(pick, total.astype(bf16), preferred_element_type=f32), 0.0).astype(bf16)
        latent = lax.dot_general(wide, wk[j], (((1,), (1,)), ((), ())), preferred_element_type=f32)
        qs[j] = latent.reshape(N, per, wide_c).astype(bf16)
        to_all(functools.partial(query_copy, j))
        qr[j, rows_of(hd * 4 + part), c_of(u)] = qs[j, pl.ds(me, 1)].reshape(per, wide_c)
        if j == 0:
            dispatch_rope()
    weight_copy(1, 1, 1).start()
    weight_copy(1, 1, 2).start()
    weight_copy(1, 1, 3).start()

    load_kv.wait()
    factor = (NOPE + R) ** -0.5
    keys = stored + 128
    sr = iota((128, 128), 0)
    sc = iota((128, 128), 1)
    half = R // 2
    swap = jnp.where((sr == sc + half) & (sc < half), -1.0, 0.0)
    swap = swap + jnp.where((sr == sc - half) & (sc >= half) & (sc < R), 1.0, 0.0)
    swap = swap.astype(bf16)
    rows = 4 * G * per
    cosines = jnp.broadcast_to(cos8[None], (4 * G, per, 128)).reshape(rows, 128)
    sines = jnp.broadcast_to(sin8[None], (4 * G, per, 128)).reshape(rows, 128)
    column = iota((rows, keys), 1)
    step_of = lax.div(lax.rem(iota((rows, keys), 0), per), own)
    shown = (column < len_ref[0]) | ((column >= stored) & (column <= stored + step_of))
    nt = (((1,), (1,)), ((), ()))

    def mixed_copy(j, ff, hh):
        p = hh * 4 + lax.rem(ff, 2) * 2 + lax.rem(lax.div(ff, 2), 2)
        return rcopy(ms.at[j, rows_of(p), c_of(lax.div(ff, 4))], mr.at[j, me], sm.at[j], rm.at[j], ff, hh)

    for j in range(U):
        got = qs.at[j, pl.ds(0, N - 1)]
        rcopy(got, got, sq.at[j], rq.at[j], f, hd).wait_recv()
        if j == 0:
            got = es_.at[pl.ds(0, near - 1)]
            rcopy(got, got, se.at[0], re_.at[0], f, hd).wait_recv()
        lat = qr[j]
        xr = er_[:, j * per:(j + 1) * per, :].astype(f32).reshape(rows, 128)
        turned = jnp.dot(xr.astype(bf16), swap, preferred_element_type=f32)
        rot = (xr * cosines + turned * sines).astype(bf16)[:, 0:R]
        s = jnp.dot(lat, kv[0:C, :], preferred_element_type=f32)
        s = s + jnp.dot(rot, kv[C:C + R, :], preferred_element_type=f32)
        n = lax.dot_general(lat, fresh[:, 0:C], nt, preferred_element_type=f32)
        n = n + lax.dot_general(rot, fresh[:, C:C + R], nt, preferred_element_type=f32)
        s = jnp.concatenate([s, n], axis=1)
        s = jnp.where(shown, s * factor, -1e30)
        m = jnp.max(s, axis=1, keepdims=True)
        w = jnp.exp(s - m)
        total = jnp.sum(w, axis=1, keepdims=True)
        w = w.astype(bf16)
        mix = lax.dot_general(w[:, 0:stored], kv[0:C, :], nt, preferred_element_type=f32)
        mix = mix + jnp.dot(w[:, stored:], fresh[:, 0:C], preferred_element_type=f32)
        ms[j] = (mix / total).astype(bf16)
        to_all(functools.partial(mixed_copy, j))
        mr[j, pl.ds(me, 1)] = ms[j, rows_of(hd * 4 + part), c_of(u)].reshape(1, per, wide_c)

    def out_copy(j, t):
        return rcopy(vs.at[j, t], vr.at[j, f], so.at[j], ro.at[j], t, hd)

    for j in range(U):
        load_uv[j].wait()
        weight_wait(1, j, "wait_recv")
        most = mr.at[j, pl.ds(0, N - 1)]
        rcopy(most, most, sm.at[j], rm.at[j], f, hd).wait_recv()
        mixed = mr[j].astype(f32).reshape(expanded, wide_c).astype(bf16)
        values = jnp.dot(mixed, wv[j], preferred_element_type=f32)
        values = jnp.where(own_head, values, 0.0).astype(bf16)
        values = lax.dot_general(pick, values, (((0,), (0,)), ((), ())), preferred_element_type=f32)
        vs[j] = values.reshape(F, steps * G, cols).astype(bf16)

        for t in spread[:-4] + spread[-3:]:
            out_copy(j, t).start()
        vr[j, pl.ds(f, 1)] = vs[j, pl.ds(f, 1)]

    for j in range(U):
        got = vs.at[j, others]
        rcopy(got, got, so.at[j], ro.at[j], f, hd).wait_recv()
        for p in range(4):
            q = (p % 2) * 2 + p // 2
            a = sum(vr[j, uu * 4 + q].astype(f32) for uu in range(U))
            for s in range(steps):
                out_ref[s, :, (p * U + j) * cols:(p * U + j + 1) * cols] = a[s * G:(s + 1) * G].astype(bf16)

    rcopy(ps.at[others], pr.at[others], sp.at[0], rp.at[0], f, hd).wait_send()
    for j in range(U):
        weight_wait(0, j, "wait_send")
        weight_wait(1, j, "wait_send")
    rcopy(pp, pv, spp.at[0], rpp.at[0], f, hd).wait_send()
    rcopy(ppr, pvr, sppr.at[0], rppr.at[0], f, hd).wait_send()
    rcopy(ls, lr, sl.at[0], rl.at[0], f, hd).wait_send()
    line_rope().wait_send()
    for j in range(U):
        each(1, U, functools.partial(half_copy, j), "wait_send")
    each(1, U, half_rope, "wait_send")
    sent = es_.at[pl.ds(0, near - 1)]
    rcopy(sent, sent, se.at[0], re_.at[0], f, hd).wait_send()
    for j in range(U):
        if True:
            sent = qs.at[j, pl.ds(0, N - 1)]
            rcopy(sent, sent, sq.at[j], rq.at[j], f, hd).wait_send()
        if True:
            sent = mr.at[j, pl.ds(0, N - 1)]
            rcopy(sent, sent, sm.at[j], rm.at[j], f, hd).wait_send()
        sent = vs.at[j, others]
        rcopy(sent, sent, so.at[j], ro.at[j], f, hd).wait_send()


def one_kernel(probe_compressed, w_uq, w_qr, w_uk, w_uv, cache, new_kv, lengths):
    F, G = lax.axis_size("fsdp"), lax.axis_size("head")
    N, U = F * G, F // 4
    steps, group, _ = probe_compressed.shape
    ck, heads = w_uk.shape[0], w_uk.shape[1] // NOPE
    own = heads // F
    C = ck * F
    queries = F * steps * G
    per = steps * own
    tall = U * per
    cols, rcols = own * NOPE, own * R
    bcols, brcols = U * cols, U * rcols
    cache = cache.transpose(0, 2, 1)
    new_kv = new_kv.transpose(1, 0, 2)
    half = R // 2
    freqs = 10000.0 ** (-(np.arange(half, dtype=np.float32) * 2.0 / R))
    freqs = np.concatenate([freqs, freqs, np.zeros(128 - R)]).astype(np.float32)[None]
    bf16 = jnp.bfloat16
    vm = lambda *shape: pltpu.VMEM(shape, bf16)
    dma = lambda *n: pltpu.SemaphoreType.DMA(n)
    vmem = pl.BlockSpec(memory_space=pltpu.VMEM)
    hbm = pl.BlockSpec(memory_space=pltpu.HBM)
    return pl.pallas_call(
        functools.partial(fused, F, G, steps, own),
        out_shape=jax.ShapeDtypeStruct((steps, group, heads * VDIM), bf16),
        in_specs=[pl.BlockSpec(memory_space=pltpu.SMEM)] + [hbm] * 8,
        out_specs=vmem,
        scratch_shapes=[
            pltpu.VMEM((1, 128), jnp.float32), vm(*probe_compressed.shape), vm(*new_kv.shape),
            vm(*w_uq.shape), vm(*w_qr.shape), vm(U, 4 * ck, cols), vm(U, 4 * ck, cols), vm(*cache.shape[1:]),
            vm(F, steps * G, w_uq.shape[0]), vm(F, steps * G, w_uq.shape[0]),
            vm(2, U, queries, cols), vm(2, U, queries, cols),
            vm(2, queries, brcols), vm(2, queries, brcols),
            vm(U, queries, cols), vm(U, queries, cols), vm(queries, brcols), vm(queries, brcols),
            vm(U, queries, cols), vm(U, U, queries, cols),
            vm(U, queries // U, brcols), vm(U, queries // U, brcols),
            vm(N // U, tall, 128), vm(4 * G, tall, 128),
            vm(U, N, per, 4 * ck), vm(U, 4 * G * per, C), vm(U, 4 * G * per, C), vm(U, N, per, 4 * ck),
            vm(U, F, steps * G, cols), vm(U, F, steps * G, cols),
            dma(7 + 2 * U), dma(1), dma(1), dma(2, U), dma(2, U), dma(1), dma(2 * U), dma(1), dma(2),
            dma(1), dma(U), dma(1), dma(1), dma(U), dma(U), dma(1), dma(1),
            dma(1), dma(1), dma(U), dma(U), dma(U), dma(U), dma(U), dma(U),
        ],
        compiler_params=pltpu.CompilerParams(
            collective_id=0, has_side_effects=True, vmem_limit_bytes=67043328
        ),
    )(lengths, jnp.asarray(freqs), probe_compressed, new_kv, w_uq, w_qr, w_uk, w_uv, cache)


def choose(*arrays):
    probe, w_uk, cache = arrays[0], arrays[3], arrays[5]
    F, G = lax.axis_size("fsdp"), lax.axis_size("head")
    own = w_uk.shape[1] // NOPE // F
    fits = own > 0 and w_uk.shape[1] == own * NOPE * F and F % 8 == 0
    fits = fits and probe.shape[1] == G and cache.shape[0] == 1
    fits = fits and (probe.shape[0] * own) % 8 == 0 and (probe.shape[0] * G) % 8 == 0
    fits = fits and w_uk.shape[0] % 16 == 0 and (4 * w_uk.shape[0]) % 128 == 0 and cache.shape[1] % 128 == 0 and (own * R) % 128 == 0
    return one_kernel(*arrays) if fits else per_device(*arrays)


def solution(mesh):
    in_specs = (
        P(None, "fsdp", None),
        P("fsdp", "head"),
        P("fsdp", "head"),
        P("fsdp", "head"),
        P("fsdp", "head"),
        P(("fsdp", "head"), None, None),
        P(None, ("fsdp", "head"), None),
        P(("fsdp", "head")),
    )
    out_specs = P(None, "fsdp", "head")
    return jax.shard_map(
        choose, mesh=mesh, in_specs=in_specs, out_specs=out_specs, check_vma=False
    )
```
